32 devices in a mesh: expert: 4 (over x, core), dp: 8 (over z, y).
Axes of the slice: x: 2, y: 2, z: 4, core: 2. Of those that a mesh axis runs over, the one named last changes fastest.
Arguments:
- tokens: bfloat16 [4096, 1024], P(('expert', 'dp')), may hold values from -6 to 6
- norm_gain: float32 [1024], replicated, may hold values from 0.1 to 1.9
- router_weight: bfloat16 [1024, 4], replicated, may hold values from -0.3984375 to 0.3984375
- shared_gate_vector: float32 [1024], replicated, may hold values from -0.4 to 0.4
- expert_ids: int32 [4096, 2], P(('expert', 'dp')), may hold values from 0 to 3, all different within a row; in each aligned block of 128 rows (0 to 127, 128 to 255, ...) at most 96 rows name the same one
- gate_weight: bfloat16 [4, 1024, 4096], P('expert', None, 'dp'), may hold values from -0.1875 to 0.1875
- up_weight: bfloat16 [4, 1024, 4096], P('expert', None, 'dp'), may hold values from -0.1875 to 0.1875
- down_weight: bfloat16 [4, 1024, 4096], P('expert', None, 'dp'), may hold values from -0.09375 to 0.09375
- shared_gate_weight: bfloat16 [1024, 4096], P(None, 'expert'), may hold values from -0.1875 to 0.1875
- shared_up_weight: bfloat16 [1024, 4096], P(None, 'expert'), may hold values from -0.1875 to 0.1875
- shared_down_weight: bfloat16 [4096, 1024], P('expert'), may hold values from -0.09375 to 0.09375
Outputs:
- mixed: bfloat16 [4096, 1024], P(('expert', 'dp'))
The draws below stay inside these ranges and needn't reach their ends.
Inputs may be any that keep to these rules, and one draw needn't show every extreme that they name: `expert_ids`: in each aligned block of 128 rows (the rows of one device) no expert is named by more than 96 pairs, and in some block one expert is named by exactly 96; the two ids of a row differ.
All inputs are finite; a program needn't handle non-finite values.
Results may differ from the reference program's by a relative error of at most 0.0085.
Values may be sent and summed in bfloat16 or wider, within the bound.
A program may use at most 128 MiB of HBM per device.

```python
import math
import jax
import jax.numpy as jnp
import numpy as np
from jax import lax

D = 1024
FF = 4096
SFF = 4096
TOK_DEV = 128
EXPERTS = 4
CAP = 96
TOKENS = 4096
N_EXPERT = 4


def shard_levels(stream_key, extent, shards, least, top_value):
    factor_of = 1.0
    for axis_at, parts in shards:
        steps = jax.random.uniform(jax.random.fold_in(jax.random.fold_in(stream_key, 6), axis_at), (parts,), jnp.float32, least / len(shards), top_value / len(shards))
        factor_of = factor_of * jnp.repeat(jnp.exp(steps), extent[axis_at] // parts).reshape((-1,) + (1,) * (len(extent) - 1 - axis_at))
    return factor_of


def routed_block(rng, own, number, rows, count, top, reach, skew):
    sequence = jax.random.permutation(rng, count)
    heavy_load, common = shares(count, rows * top, reach, skew, True), shares(count, rows * top, reach, skew, False)
    places = jnp.arange(count)

    def named(tallies, rotation):
        used = int((tallies > 0).sum())
        fixed = max(1, used // 4)
        shifted = fixed + (places - fixed + rotation * (used - fixed)) % max(1, count - fixed)
        return jnp.zeros((count,), jnp.int32).at[sequence[jnp.where(places < fixed, places, shifted)]].set(jnp.asarray(tallies, jnp.int32))

    tallies = jnp.where(number % 4 == 0, named(heavy_load, number // 4), named(common, number - number // 4 - 1))
    mixed = jax.random.permutation(jax.random.fold_in(own, 3), count)
    donor, receiver = mixed[0:count // 2 * 2:2], mixed[1:count // 2 * 2:2]
    room = jnp.minimum(tallies[donor] - 1, reach - tallies[receiver]) // 2
    room = jnp.where((donor == sequence[0]) | (receiver == sequence[0]) | (tallies[receiver] == 0), 0, jnp.maximum(room, 0))
    shifted = jax.random.randint(jax.random.fold_in(own, 4), (count // 2,), 0, 1 << 20) % (room + 1)
    tallies = tallies.at[donor].add(-shifted).at[receiver].add(shifted)
    items = jnp.searchsorted(jnp.cumsum(tallies), jnp.arange(rows * top), side="right").astype(jnp.int32)
    listing = items.reshape(top, rows).T
    listing = listing[jax.random.permutation(jax.random.fold_in(own, 1), rows)]
    rotation = jax.random.randint(jax.random.fold_in(own, 2), (rows, 1), 0, top)
    return jnp.take_along_axis(listing, (jnp.arange(top)[None, :] + rotation) % top, axis=1)


def shares(number_of, total, bound, lean, full):
    portions = [(1 << 20) // math.isqrt(rank ** lean) + 1 for rank in range(1, number_of + 1)]
    largest = bound if full else min(bound, max(-(-total // number_of), total * portions[0] // sum(portions)))
    least = 1 if total - largest >= number_of - 1 else 0
    holding, surplus = [largest] + [least] * (number_of - 1), total - largest - least * (number_of - 1)
    while surplus > 0:
        movable = [i for i in range(1, number_of) if holding[i] < largest] or [i for i in range(1, number_of) if holding[i] < bound]
        mass, remaining = sum([portions[i] for i in movable]), surplus
        for i in movable:
            addition = min(bound - holding[i], max(1, remaining * portions[i] // mass), surplus)
            holding[i] = holding[i] + addition
            surplus = surplus - addition
    return np.array(holding)


def bell_draw(own_key, shape, spread, limit, cuts=(), kind=jnp.bfloat16):
    values = spread * jax.random.normal(own_key, shape, jnp.float32)
    if cuts:
        values = values * shard_levels(own_key, shape, cuts, -0.22, 0.18)
    return jnp.clip(values, -limit, limit).astype(kind)


def setup_inputs(seed: int = 0) -> dict:
    arg_keys = jax.random.split(jax.random.key(seed), 12)
    tokens = bell_draw(arg_keys[0], (TOKENS, D), 1.0, 6.0, ((0, 32),))
    norm_gain = jnp.clip(1.0 + 0.18 * jax.random.normal(arg_keys[1], (D,), jnp.float32), 0.1, 1.9)
    router_weight = bell_draw(arg_keys[2], (D, EXPERTS), 0.0625, 0.3984375)
    shared_gate_vector = bell_draw(arg_keys[3], (D,), 0.0625, 0.4, (), jnp.float32)
    expert_ids_keys = jax.random.split(jax.random.fold_in(arg_keys[4], 1), TOKENS // TOK_DEV)
    expert_ids_turns = jax.random.permutation(jax.random.fold_in(arg_keys[4], 3), TOKENS // TOK_DEV)
    expert_ids = jax.vmap(lambda own, number: routed_block(jax.random.fold_in(arg_keys[4], 2), own, number, TOK_DEV, EXPERTS, 2, CAP, 2))(expert_ids_keys, expert_ids_turns).reshape((TOKENS, 2))
    gate_weight = bell_draw(arg_keys[5], (EXPERTS, D, FF), D ** -0.5, 0.1875, ((0, 4), (2, 8)))
    up_weight = bell_draw(arg_keys[6], (EXPERTS, D, FF), D ** -0.5, 0.1875, ((0, 4), (2, 8)))
    down_weight = bell_draw(arg_keys[7], (EXPERTS, D, FF), FF ** -0.5, 0.09375, ((0, 4), (2, 8)))
    shared_gate_weight = bell_draw(arg_keys[8], (D, SFF), D ** -0.5, 0.1875, ((1, 4),))
    shared_up_weight = bell_draw(arg_keys[9], (D, SFF), D ** -0.5, 0.1875, ((1, 4),))
    shared_down_weight = bell_draw(arg_keys[10], (SFF, D), SFF ** -0.5, 0.09375, ((0, 4),))
    return dict(tokens=tokens, norm_gain=norm_gain, router_weight=router_weight, shared_gate_vector=shared_gate_vector, expert_ids=expert_ids, gate_weight=gate_weight, up_weight=up_weight, down_weight=down_weight, shared_gate_weight=shared_gate_weight, shared_up_weight=shared_up_weight, shared_down_weight=shared_down_weight)


def rms_norm(values, gain):
    floats = values.astype(jnp.float32)
    mean_square = lax.optimization_barrier(jnp.mean(floats * floats, axis=-1, keepdims=True))
    return (floats * lax.rsqrt(mean_square + 1e-06) * gain).astype(jnp.bfloat16)

def routing(normed, router_weight, expert_ids):
    logits = jnp.dot(normed, router_weight, preferred_element_type=jnp.float32)
    onehot = expert_ids[:, :, None] == jnp.arange(router_weight.shape[1], dtype=jnp.int32)[None, None, :]
    picked = lax.optimization_barrier(jnp.sum(jnp.where(onehot, logits[:, None, :], jnp.float32(0.0)), axis=-1))
    first_weight = jax.nn.sigmoid(picked[:, 0] - picked[:, 1])
    return jnp.stack([first_weight, 1.0 - first_weight], axis=1)

def slot_of(block_ids):
    flat_ids = block_ids.reshape(-1)
    onehot = (flat_ids[:, None] == jnp.arange(EXPERTS, dtype=jnp.int32)[None, :]).astype(jnp.int32)
    before = jnp.cumsum(onehot, axis=0) - onehot
    return lax.optimization_barrier(jnp.sum(before * onehot, axis=1)).reshape(block_ids.shape).astype(jnp.int32)

def reference(tokens, norm_gain, router_weight, shared_gate_vector, expert_ids, gate_weight, up_weight, down_weight, shared_gate_weight, shared_up_weight, shared_down_weight):
    normed = rms_norm(tokens, norm_gain)
    route_weight = routing(normed, router_weight, expert_ids)
    num_blocks = TOKENS // TOK_DEV
    slot = jax.vmap(slot_of)(expert_ids.reshape(num_blocks, TOK_DEV, 2)).reshape(TOKENS, 2)
    source_block = (jnp.arange(TOKENS, dtype=jnp.int32) // TOK_DEV).astype(jnp.int32)
    position = (source_block[:, None] * CAP + slot).astype(jnp.int32)
    padded_rows = num_blocks * CAP

    def expert_step(running, expert_index):
        slot_index = jnp.where(expert_ids == expert_index, position, padded_rows).astype(jnp.int32)
        buffer = jnp.zeros((padded_rows, D), jnp.bfloat16)
        buffer = buffer.at[slot_index[:, 0]].set(normed, mode='drop')
        buffer = buffer.at[slot_index[:, 1]].set(normed, mode='drop')
        gate_part = jnp.dot(buffer, gate_weight[expert_index], preferred_element_type=jnp.float32)
        up_part = jnp.dot(buffer, up_weight[expert_index], preferred_element_type=jnp.float32)
        hidden = (jax.nn.silu(gate_part) * up_part).astype(jnp.bfloat16)
        expert_out = lax.dot_general(hidden, down_weight[expert_index], (((1,), (1,)), ((), ())), preferred_element_type=jnp.float32).astype(jnp.bfloat16)
        for column in range(2):
            fetched = expert_out[jnp.minimum(slot_index[:, column], padded_rows - 1)].astype(jnp.float32)
            scale = jnp.where(expert_ids[:, column] == expert_index, route_weight[:, column], jnp.float32(0.0))
            running = running + scale[:, None] * fetched
        return (running, None)
    routed, _ = lax.scan(expert_step, jnp.zeros((TOKENS, D), jnp.float32), jnp.arange(EXPERTS, dtype=jnp.int32))
    block_units = SFF // N_EXPERT
    shared = jnp.zeros((TOKENS, D), jnp.float32)
    for block_index in range(N_EXPERT):
        lower = block_index * block_units
        gate_part = jnp.dot(normed, shared_gate_weight[:, lower:lower + block_units], preferred_element_type=jnp.float32)
        up_part = jnp.dot(normed, shared_up_weight[:, lower:lower + block_units], preferred_element_type=jnp.float32)
        hidden = (jax.nn.silu(gate_part) * up_part).astype(jnp.bfloat16)
        partial_out = jnp.dot(hidden, shared_down_weight[lower:lower + block_units, :], preferred_element_type=jnp.float32).astype(jnp.bfloat16)
        partial_out = lax.optimization_barrier(partial_out)
        shared = shared + partial_out.astype(jnp.float32)
    shared_gate = jax.nn.sigmoid(lax.optimization_barrier(jnp.sum(normed.astype(jnp.float32) * shared_gate_vector, axis=-1)))
    return (routed + shared_gate[:, None] * shared).astype(jnp.bfloat16)
```

```python
import functools

import jax
import jax.numpy as jnp
from jax import lax
from jax.experimental import pallas as pl
from jax.experimental.pallas import tpu as pltpu
from jax.sharding import PartitionSpec as P


def rms_norm(values, gain):
    floats = values.astype(jnp.float32)
    mean_square = jnp.mean(floats * floats, axis=-1, keepdims=True)
    return (floats * lax.rsqrt(mean_square + 1e-06) * gain).astype(jnp.bfloat16)


def routing(normed, router_weight, expert_ids):
    logits = jnp.dot(normed, router_weight, preferred_element_type=jnp.float32)
    onehot = (
        expert_ids[:, :, None] == jnp.arange(router_weight.shape[1], dtype=jnp.int32)[None, None, :]
    )
    picked = jnp.sum(jnp.where(onehot, logits[:, None, :], jnp.float32(0.0)), axis=-1)
    first_weight = jax.nn.sigmoid(picked[:, 0] - picked[:, 1])
    return jnp.stack([first_weight, 1.0 - first_weight], axis=1)


def slot_of(block_ids, experts):
    flat_ids = block_ids.reshape(-1)
    onehot = (flat_ids[:, None] == jnp.arange(experts, dtype=jnp.int32)[None, :]).astype(jnp.int32)
    before = jnp.cumsum(onehot, axis=0) - onehot
    return jnp.sum(before * onehot, axis=1).reshape(block_ids.shape)


def swiglu_hidden(inputs, gate_piece, up_piece):
    gate_part = jnp.dot(inputs, gate_piece, preferred_element_type=jnp.float32)
    up_part = jnp.dot(inputs, up_piece, preferred_element_type=jnp.float32)
    return (jax.nn.silu(gate_part) * up_part).astype(jnp.bfloat16)


def down_product(hidden, down_piece):
    return lax.dot_general(
        hidden, down_piece, (((1,), (1,)), ((), ())), preferred_element_type=jnp.float32
    )


def body(
    tokens,
    norm_gain,
    router_weight,
    shared_gate_vector,
    expert_ids,
    gate_weight,
    up_weight,
    down_weight,
    shared_gate_weight,
    shared_up_weight,
    shared_down_weight,
):
    experts = lax.axis_size("expert")
    tok_rows = tokens.shape[0]
    width = tokens.shape[1]
    capacity = 3 * tok_rows // experts
    normed = rms_norm(tokens, norm_gain)
    route_weight = routing(normed, router_weight, expert_ids)
    slot = slot_of(expert_ids, experts)
    target = expert_ids * capacity + slot
    slot_iota = jnp.arange(experts * capacity, dtype=jnp.int32)[:, None]
    dispatch_table = (
        (target[:, 0][None, :] == slot_iota) | (target[:, 1][None, :] == slot_iota)
    ).astype(jnp.bfloat16)
    outgoing = jnp.dot(dispatch_table, normed, preferred_element_type=jnp.float32).astype(
        jnp.bfloat16
    )
    outgoing = outgoing.reshape(experts, capacity, width)
    arrived = lax.all_to_all(outgoing, "expert", split_axis=0, concat_axis=0, tiled=True).reshape(
        experts * capacity, width
    )
    hidden = swiglu_hidden(
        arrived,
        lax.all_gather(gate_weight, "dp", axis=2, tiled=True)[0],
        lax.all_gather(up_weight, "dp", axis=2, tiled=True)[0],
    )
    hidden_all = hidden
    hidden = hidden_all
    expert_out = down_product(hidden, lax.all_gather(down_weight, "dp", axis=2, tiled=True)[0])
    expert_out = expert_out.astype(jnp.bfloat16).reshape(experts, capacity, width)
    returned_rows = lax.all_to_all(
        expert_out, "expert", split_axis=0, concat_axis=0, tiled=True
    ).reshape(experts * capacity, width)
    fetched = returned_rows[target].astype(jnp.float32)
    routed = jnp.sum(route_weight[:, :, None] * fetched, axis=1)
    gathered = lax.all_gather(normed, "expert", axis=0, tiled=True)
    hidden = swiglu_hidden(gathered, shared_gate_weight, shared_up_weight)
    shared = lax.psum_scatter(
        jnp.dot(hidden, shared_down_weight, preferred_element_type=jnp.float32).astype(
            jnp.bfloat16
        ),
        "expert",
        scatter_dimension=0,
        tiled=True,
    ).astype(jnp.float32)
    shared_gate = jax.nn.sigmoid(jnp.sum(normed.astype(jnp.float32) * shared_gate_vector, axis=-1))
    return (routed + shared_gate[:, None] * shared).astype(jnp.bfloat16)

NONE, X, Y, XY = 0, 1, 2, 3
Z0, Z1, Z2, Z12 = 0, 1, 2, 3
VMEM_LIMIT = 62 * 1024 * 1024
CHUNK = 256


def flipped(position, bit):
    return position + bit - 2 * bit * ((position // bit) % 2)


def fused_kernel(
    rows,
    hidden_units,
    shared_units,
    normed_ref,
    scale_ref,
    gate_ref,
    up_ref,
    down_ref,
    sgate_ref,
    sup_ref,
    sdown_ref,
    out_ref,
    tok,
    sc,
    part,
    from_core,
    from_diag,
    from_x,
    from_y,
    from_z,
    w_gate,
    w_up,
    down_raw,
    w_down,
    send_sem,
    recv_sem,
    load_sem,
):
    e_at = lax.axis_index("expert")
    d_at = lax.axis_index("dp")
    partner = {
        "c": (flipped(e_at, 1), d_at),
        "x": (flipped(e_at, 2), d_at),
        "y": (e_at, flipped(d_at, 1)),
        "z1": (e_at, flipped(d_at, 2)),
        "z2": (e_at, flipped(d_at, 4)),
    }
    half = rows // 2
    messages = {}

    def send(name, src, dst, to):
        at = len(messages)
        copy = pltpu.make_async_remote_copy(
            src_ref=src,
            dst_ref=dst,
            send_sem=send_sem.at[at],
            recv_sem=recv_sem.at[at],
            device_id=partner[to],
            device_id_type=pl.DeviceIdType.MESH,
        )
        copy.start()
        messages[name] = copy

    def arrive(name):
        messages[name].wait_recv()

    first = pl.multiple_of(d_at * shared_units, shared_units)
    loads = [
        pltpu.make_async_copy(gate_ref.at[0], w_gate.at[:, pl.ds(0, hidden_units)], load_sem.at[0]),
        pltpu.make_async_copy(up_ref.at[0], w_up.at[:, pl.ds(0, hidden_units)], load_sem.at[1]),
        pltpu.make_async_copy(
            sgate_ref.at[:, pl.ds(first, shared_units)],
            w_gate.at[:, pl.ds(hidden_units, shared_units)],
            load_sem.at[2],
        ),
        pltpu.make_async_copy(
            sup_ref.at[:, pl.ds(first, shared_units)],
            w_up.at[:, pl.ds(hidden_units, shared_units)],
            load_sem.at[3],
        ),
        pltpu.make_async_copy(
            sdown_ref.at[pl.ds(first, shared_units), :],
            w_down.at[pl.ds(hidden_units, shared_units), :],
            load_sem.at[4],
        ),
        pltpu.make_async_copy(down_ref.at[0], down_raw, load_sem.at[5]),
        pltpu.make_async_copy(normed_ref, tok.at[0, 0], load_sem.at[6]),
        pltpu.make_async_copy(scale_ref, sc.at[0, 0], load_sem.at[7]),
    ]
    loads[6].start()
    loads[7].start()
    for load in loads[:6]:
        load.start()

    barrier = pltpu.get_barrier_semaphore()
    for to in partner.values():
        pl.semaphore_signal(
            barrier, inc=1, device_id=to, device_id_type=pl.DeviceIdType.MESH
        )
    pl.semaphore_wait(barrier, len(partner))

    def slot(z, xy):
        return 4 * z + xy

    def send_tokens(kind, z_from, xy_from, z_to, xy_to, to):
        send((kind, z_to, xy_to), tok.at[slot(z_from, xy_from), 0], tok.at[slot(z_to, xy_to), 0], to)
        send(
            (kind + "s", z_to, xy_to), sc.at[slot(z_from, xy_from), 0], sc.at[slot(z_to, xy_to), 0], to
        )

    def tokens_arrive(kind, z, xy):
        arrive((kind, z, xy))
        arrive((kind + "s", z, xy))

    def share(z, xy):
        at = slot(z, xy)
        send(("c", z, xy), tok.at[at, 0], tok.at[at, 1], "c")
        send(("cs", z, xy), sc.at[at, 0], sc.at[at, 1], "c")

    def spread(z):
        send_tokens("g", z, NONE, z, X, "x")
        send_tokens("g", z, NONE, z, Y, "y")
        share(z, NONE)

    def diagonal(z):
        tokens_arrive("g", z, X)
        tokens_arrive("g", z, Y)
        low, high = pl.ds(0, half), pl.ds(half, half)
        send(
            ("lo", z), tok.at[slot(z, Y), 0, low], tok.at[slot(z, XY), 0, low], "x"
        )
        send(
            ("hi", z), tok.at[slot(z, X), 0, high], tok.at[slot(z, XY), 0, high], "y"
        )
        send(("ds", z), sc.at[slot(z, X), 0], sc.at[slot(z, XY), 0], "y")
        share(z, X)
        share(z, Y)

    def diagonal_arrives(z):
        arrive(("lo", z))
        arrive(("hi", z))
        arrive(("ds", z))
        share(z, XY)

    def compute(z, xy):
        arrive(("c", z, xy))
        arrive(("cs", z, xy))
        at = slot(z, xy)
        lane = lax.broadcasted_iota(jnp.int32, (rows, sc.shape[2]), 1)
        routed_scale, shared_scale = [], []
        for core in range(2):
            columns = jnp.transpose(sc[at, core])
            routed_scale.append(
                jnp.sum(jnp.where(lane == e_at, columns, 0.0), axis=1, keepdims=True)
            )
            shared_scale.append(columns[:, sc.shape[2] - 1 :])
        routed_scale = jnp.concatenate(routed_scale, axis=0)
        shared_scale = jnp.concatenate(shared_scale, axis=0)
        inputs = tok[at].reshape(2 * rows, tok.shape[3])
        gate_part = jnp.dot(inputs, w_gate[...], preferred_element_type=jnp.float32)
        up_part = jnp.dot(inputs, w_up[...], preferred_element_type=jnp.float32)
        hidden = gate_part * jax.nn.sigmoid(gate_part) * up_part
        hidden = jnp.concatenate(
            [
                (hidden[:, :hidden_units] * routed_scale).astype(jnp.bfloat16),
                (hidden[:, hidden_units:] * shared_scale).astype(jnp.bfloat16),
            ],
            axis=1,
        )
        result = jnp.dot(hidden, w_down[...], preferred_element_type=jnp.float32)
        part[at] = result.astype(jnp.bfloat16).reshape(2, rows, tok.shape[3])
        send(("pc", z, xy), part.at[at, 1], from_core.at[at], "c")

    def f32(values):
        return values.astype(jnp.float32)

    def chip_sum(z, xy):
        arrive(("pc", z, xy))
        return f32(part[slot(z, xy), 0]) + f32(from_core[slot(z, xy)])

    def send_diagonal(z):
        at = slot(z, XY)
        part[at, 0] = chip_sum(z, XY).astype(jnp.bfloat16)
        low, high = pl.ds(0, half), pl.ds(half, half)
        send(("plo", z), part.at[at, 0, low], from_diag.at[z, low], "x")
        send(("phi", z), part.at[at, 0, high], from_diag.at[z, high], "y")

    def send_sides(z):
        arrive(("plo", z))
        arrive(("phi", z))
        total = chip_sum(z, X)
        part[slot(z, X), 0, :half] = total[:half].astype(jnp.bfloat16)
        part[slot(z, X), 0, half:] = (total[half:] + f32(from_diag[z, half:])).astype(jnp.bfloat16)
        send(("px", z), part.at[slot(z, X), 0], from_x.at[z], "x")
        total = chip_sum(z, Y)
        part[slot(z, Y), 0, :half] = (total[:half] + f32(from_diag[z, :half])).astype(jnp.bfloat16)
        part[slot(z, Y), 0, half:] = total[half:].astype(jnp.bfloat16)
        send(("py", z), part.at[slot(z, Y), 0], from_y.at[z], "y")

    def column_sum(z):
        total = chip_sum(z, NONE)
        arrive(("px", z))
        arrive(("py", z))
        return total + f32(from_x[z]) + f32(from_y[z])

    loads[6].wait()
    loads[7].wait()
    send_tokens("g", Z0, NONE, Z1, NONE, "z1")
    spread(Z0)
    send_tokens("g", Z0, NONE, Z2, NONE, "z2")
    for load in loads[:6]:
        load.wait()
    w_down[0:hidden_units, :] = jnp.transpose(down_raw[...])

    order = (Z0, Z1, Z2, Z12)
    for number, z in enumerate(order):
        compute(z, NONE)
        diagonal(z)
        if number + 1 < len(order):
            later = order[number + 1]
            tokens_arrive("g", later, NONE)
            if later == Z2:
                send_tokens("g", Z2, NONE, Z12, NONE, "z1")
            spread(later)
        compute(z, X)
        compute(z, Y)
        diagonal_arrives(z)
        compute(z, XY)
        if number:
            send_diagonal(order[number - 1])
    send_diagonal(Z12)

    send_sides(Z12)
    send_sides(Z2)
    part[slot(Z12, NONE), 0] = column_sum(Z12).astype(jnp.bfloat16)
    send(("pz", Z12), part.at[slot(Z12, NONE), 0], from_z.at[0], "z1")
    send_sides(Z1)
    total = column_sum(Z2)
    arrive(("pz", Z12))
    part[slot(Z2, NONE), 0] = (total + f32(from_z[0])).astype(jnp.bfloat16)
    send(("pz", Z2), part.at[slot(Z2, NONE), 0], from_z.at[1], "z2")
    send_sides(Z0)
    part[slot(Z1, NONE), 0] = column_sum(Z1).astype(jnp.bfloat16)
    send(("pz", Z1), part.at[slot(Z1, NONE), 0], from_z.at[2], "z1")
    total = column_sum(Z0)
    arrive(("pz", Z2))
    arrive(("pz", Z1))
    out_ref[...] = (total + f32(from_z[1]) + f32(from_z[2])).astype(out_ref.dtype)
    for copy in messages.values():
        copy.wait_send()


MESSAGES = 112


def fused_body(
    tokens,
    norm_gain,
    router_weight,
    shared_gate_vector,
    expert_ids,
    gate_weight,
    up_weight,
    down_weight,
    shared_gate_weight,
    shared_up_weight,
    shared_down_weight,
):
    experts = lax.axis_size("expert")
    rows, width = tokens.shape
    hidden_units = gate_weight.shape[2]
    shared_units = shared_gate_weight.shape[1] // lax.axis_size("dp")
    normed = rms_norm(tokens, norm_gain)
    route_weight = routing(normed, router_weight, expert_ids)
    shared_gate = jax.nn.sigmoid(jnp.sum(normed.astype(jnp.float32) * shared_gate_vector, axis=-1))
    expert_iota = jnp.arange(experts, dtype=jnp.int32)[:, None]
    by_expert = jnp.where(
        expert_ids[:, 0][None, :] == expert_iota, route_weight[:, 0][None, :], 0.0
    ) + jnp.where(expert_ids[:, 1][None, :] == expert_iota, route_weight[:, 1][None, :], 0.0)
    scales = jnp.concatenate(
        [by_expert, jnp.broadcast_to(shared_gate[None, :], (8 - experts, rows))], axis=0
    )
    units = hidden_units + shared_units
    planes = 16
    anywhere = pl.BlockSpec(memory_space=pl.ANY)
    block = (rows, width)
    return pl.pallas_call(
        functools.partial(fused_kernel, rows, hidden_units, shared_units),
        out_shape=jax.ShapeDtypeStruct(block, jnp.bfloat16),
        in_specs=[anywhere] * 8,
        out_specs=pl.BlockSpec(memory_space=pltpu.VMEM),
        scratch_shapes=[
            pltpu.VMEM((planes, 2) + block, jnp.bfloat16),
            pltpu.VMEM((planes, 2, 8, rows), jnp.float32),
            pltpu.VMEM((planes, 2) + block, jnp.bfloat16),
            pltpu.VMEM((planes,) + block, jnp.bfloat16),
            pltpu.VMEM((4,) + block, jnp.bfloat16),
            pltpu.VMEM((4,) + block, jnp.bfloat16),
            pltpu.VMEM((4,) + block, jnp.bfloat16),
            pltpu.VMEM((3,) + block, jnp.bfloat16),
            pltpu.VMEM((width, units), jnp.bfloat16),
            pltpu.VMEM((width, units), jnp.bfloat16),
            pltpu.VMEM((width, hidden_units), jnp.bfloat16),
            pltpu.VMEM((units, width), jnp.bfloat16),
            pltpu.SemaphoreType.DMA((MESSAGES,)),
            pltpu.SemaphoreType.DMA((MESSAGES,)),
            pltpu.SemaphoreType.DMA((8,)),
        ],
        compiler_params=pltpu.CompilerParams(
            collective_id=0, has_side_effects=True, vmem_limit_bytes=VMEM_LIMIT
        ),
    )(
        normed,
        scales,
        gate_weight,
        up_weight,
        down_weight,
        shared_gate_weight,
        shared_up_weight,
        shared_down_weight,
    )


def solution(mesh):
    fused = mesh.shape["expert"] == 4 and mesh.shape["dp"] == 8
    return jax.shard_map(
        fused_body if fused else body,
        mesh=mesh,
        in_specs=(
            P(("expert", "dp"), None),
            P(),
            P(),
            P(),
            P(("expert", "dp"), None),
            P("expert", None, "dp"),
            P("expert", None, "dp"),
            P("expert", None, "dp"),
            P(None, "expert"),
            P(None, "expert"),
            P("expert", None),
        ),
        out_specs=P(("expert", "dp"), None),
        check_vma=False,
    )
```

```python
import functools

import jax
import jax.numpy as jnp
from jax import lax
from jax.experimental import pallas as pl
from jax.experimental.pallas import tpu as pltpu
from jax.sharding import PartitionSpec as P


def rms_norm(values, gain):
    floats = values.astype(jnp.float32)
    mean_square = jnp.mean(floats * floats, axis=-1, keepdims=True)
    return (floats * lax.rsqrt(mean_square + 1e-06) * gain).astype(jnp.bfloat16)


def routing(normed, router_weight, expert_ids):
    logits = jnp.dot(normed, router_weight, preferred_element_type=jnp.float32)
    onehot = (
        expert_ids[:, :, None] == jnp.arange(router_weight.shape[1], dtype=jnp.int32)[None, None, :]
    )
    picked = jnp.sum(jnp.where(onehot, logits[:, None, :], jnp.float32(0.0)), axis=-1)
    first_weight = jax.nn.sigmoid(picked[:, 0] - picked[:, 1])
    return jnp.stack([first_weight, 1.0 - first_weight], axis=1)


def slot_of(block_ids, experts):
    flat_ids = block_ids.reshape(-1)
    onehot = (flat_ids[:, None] == jnp.arange(experts, dtype=jnp.int32)[None, :]).astype(jnp.int32)
    before = jnp.cumsum(onehot, axis=0) - onehot
    return jnp.sum(before * onehot, axis=1).reshape(block_ids.shape)


def swiglu_hidden(inputs, gate_piece, up_piece):
    gate_part = jnp.dot(inputs, gate_piece, preferred_element_type=jnp.float32)
    up_part = jnp.dot(inputs, up_piece, preferred_element_type=jnp.float32)
    return (jax.nn.silu(gate_part) * up_part).astype(jnp.bfloat16)


def down_product(hidden, down_piece):
    return lax.dot_general(
        hidden, down_piece, (((1,), (1,)), ((), ())), preferred_element_type=jnp.float32
    )


def body(
    tokens,
    norm_gain,
    router_weight,
    shared_gate_vector,
    expert_ids,
    gate_weight,
    up_weight,
    down_weight,
    shared_gate_weight,
    shared_up_weight,
    shared_down_weight,
):
    experts = lax.axis_size("expert")
    tok_rows = tokens.shape[0]
    width = tokens.shape[1]
    capacity = 3 * tok_rows // experts
    normed = rms_norm(tokens, norm_gain)
    route_weight = routing(normed, router_weight, expert_ids)
    slot = slot_of(expert_ids, experts)
    target = expert_ids * capacity + slot
    slot_iota = jnp.arange(experts * capacity, dtype=jnp.int32)[:, None]
    dispatch_table = (
        (target[:, 0][None, :] == slot_iota) | (target[:, 1][None, :] == slot_iota)
    ).astype(jnp.bfloat16)
    outgoing = jnp.dot(dispatch_table, normed, preferred_element_type=jnp.float32).astype(
        jnp.bfloat16
    )
    outgoing = outgoing.reshape(experts, capacity, width)
    arrived = lax.all_to_all(outgoing, "expert", split_axis=0, concat_axis=0, tiled=True).reshape(
        experts * capacity, width
    )
    hidden = swiglu_hidden(
        arrived,
        lax.all_gather(gate_weight, "dp", axis=2, tiled=True)[0],
        lax.all_gather(up_weight, "dp", axis=2, tiled=True)[0],
    )
    hidden_all = hidden
    hidden = hidden_all
    expert_out = down_product(hidden, lax.all_gather(down_weight, "dp", axis=2, tiled=True)[0])
    expert_out = expert_out.astype(jnp.bfloat16).reshape(experts, capacity, width)
    returned_rows = lax.all_to_all(
        expert_out, "expert", split_axis=0, concat_axis=0, tiled=True
    ).reshape(experts * capacity, width)
    fetched = returned_rows[target].astype(jnp.float32)
    routed = jnp.sum(route_weight[:, :, None] * fetched, axis=1)
    gathered = lax.all_gather(normed, "expert", axis=0, tiled=True)
    hidden = swiglu_hidden(gathered, shared_gate_weight, shared_up_weight)
    shared = lax.psum_scatter(
        jnp.dot(hidden, shared_down_weight, preferred_element_type=jnp.float32).astype(
            jnp.bfloat16
        ),
        "expert",
        scatter_dimension=0,
        tiled=True,
    ).astype(jnp.float32)
    shared_gate = jax.nn.sigmoid(jnp.sum(normed.astype(jnp.float32) * shared_gate_vector, axis=-1))
    return (routed + shared_gate[:, None] * shared).astype(jnp.bfloat16)

NONE, X, Y, XY = 0, 1, 2, 3
Z0, Z1, Z2, Z12 = 0, 1, 2, 3
VMEM_LIMIT = 62 * 1024 * 1024


def flipped(position, bit):
    return position + bit - 2 * bit * ((position // bit) % 2)


def fused_kernel(
    rows,
    hidden_units,
    shared_units,
    tokens_ref,
    gain_ref,
    router_ref,
    vector_ref,
    ids_ref,
    gate_ref,
    up_ref,
    down_ref,
    sgate_ref,
    sup_ref,
    sdown_ref,
    out_ref,
    tok,
    sc,
    part,
    from_core,
    from_diag,
    from_x,
    from_y,
    from_z,
    w_gate,
    w_up,
    down_raw,
    w_down,
    send_sem,
    recv_sem,
    load_sem,
):
    e_at = lax.axis_index("expert")
    d_at = lax.axis_index("dp")
    partner = {
        "c": (flipped(e_at, 1), d_at),
        "x": (flipped(e_at, 2), d_at),
        "y": (e_at, flipped(d_at, 1)),
        "z1": (e_at, flipped(d_at, 2)),
        "z2": (e_at, flipped(d_at, 4)),
    }
    half = rows // 2
    messages = {}

    def send(name, src, dst, to):
        at = len(messages)
        copy = pltpu.make_async_remote_copy(
            src_ref=src,
            dst_ref=dst,
            send_sem=send_sem.at[at],
            recv_sem=recv_sem.at[at],
            device_id=partner[to],
            device_id_type=pl.DeviceIdType.MESH,
        )
        copy.start()
        messages[name] = copy

    def arrive(name):
        messages[name].wait_recv()

    first = pl.multiple_of(d_at * shared_units, shared_units)
    loads = [
        pltpu.make_async_copy(gate_ref.at[0], w_gate.at[:, pl.ds(0, hidden_units)], load_sem.at[0]),
        pltpu.make_async_copy(up_ref.at[0], w_up.at[:, pl.ds(0, hidden_units)], load_sem.at[1]),
        pltpu.make_async_copy(
            sgate_ref.at[:, pl.ds(first, shared_units)],
            w_gate.at[:, pl.ds(hidden_units, shared_units)],
            load_sem.at[2],
        ),
        pltpu.make_async_copy(
            sup_ref.at[:, pl.ds(first, shared_units)],
            w_up.at[:, pl.ds(hidden_units, shared_units)],
            load_sem.at[3],
        ),
        pltpu.make_async_copy(
            sdown_ref.at[pl.ds(first, shared_units), :],
            w_down.at[pl.ds(hidden_units, shared_units), :],
            load_sem.at[4],
        ),
        pltpu.make_async_copy(down_ref.at[0], down_raw, load_sem.at[5]),
    ]
    for load in loads:
        load.start()

    barrier = pltpu.get_barrier_semaphore()
    for to in partner.values():
        pl.semaphore_signal(
            barrier, inc=1, device_id=to, device_id_type=pl.DeviceIdType.MESH
        )

    floats = tokens_ref[...].astype(jnp.float32)
    mean_square = jnp.mean(floats * floats, axis=-1, keepdims=True)
    normed = (floats * lax.rsqrt(mean_square + 1e-06) * gain_ref[...][None, :]).astype(jnp.bfloat16)
    tok[0, 0] = normed
    logits = jnp.dot(normed, router_ref[...], preferred_element_type=jnp.float32)
    ids = ids_ref[...]
    first_id, second_id = ids[:, 0:1], ids[:, 1:2]
    column = lax.broadcasted_iota(jnp.int32, logits.shape, 1)
    margin = jnp.sum(
        jnp.where(column == first_id, logits, 0.0), axis=1, keepdims=True
    ) - jnp.sum(jnp.where(column == second_id, logits, 0.0), axis=1, keepdims=True)
    first_weight = jax.nn.sigmoid(margin)
    shared_gate = jax.nn.sigmoid(
        jnp.sum(normed.astype(jnp.float32) * vector_ref[...][None, :], axis=-1, keepdims=True)
    )
    column = lax.broadcasted_iota(jnp.int32, (rows, sc.shape[2]), 1)
    scales = jnp.where(column == first_id, first_weight, 0.0)
    scales = scales + jnp.where(column == second_id, 1.0 - first_weight, 0.0)
    scales = scales + jnp.where(column == sc.shape[2] - 1, shared_gate, 0.0)
    sc[0, 0] = jnp.transpose(scales)
    pl.semaphore_wait(barrier, len(partner))

    def slot(z, xy):
        return 4 * z + xy

    def send_tokens(kind, z_from, xy_from, z_to, xy_to, to):
        send((kind, z_to, xy_to), tok.at[slot(z_from, xy_from), 0], tok.at[slot(z_to, xy_to), 0], to)
        send(
            (kind + "s", z_to, xy_to), sc.at[slot(z_from, xy_from), 0], sc.at[slot(z_to, xy_to), 0], to
        )

    def tokens_arrive(kind, z, xy):
        arrive((kind, z, xy))
        arrive((kind + "s", z, xy))

    def share(z, xy):
        at = slot(z, xy)
        send(("c", z, xy), tok.at[at, 0], tok.at[at, 1], "c")
        send(("cs", z, xy), sc.at[at, 0], sc.at[at, 1], "c")

    def spread(z):
        send_tokens("g", z, NONE, z, X, "x")
        send_tokens("g", z, NONE, z, Y, "y")
        share(z, NONE)

    def diagonal(z):
        tokens_arrive("g", z, X)
        tokens_arrive("g", z, Y)
        low, high = pl.ds(0, half), pl.ds(half, half)
        send(
            ("lo", z), tok.at[slot(z, Y), 0, low], tok.at[slot(z, XY), 0, low], "x"
        )
        send(
            ("hi", z), tok.at[slot(z, X), 0, high], tok.at[slot(z, XY), 0, high], "y"
        )
        send(("ds", z), sc.at[slot(z, X), 0], sc.at[slot(z, XY), 0], "y")
        share(z, X)
        share(z, Y)

    def diagonal_arrives(z):
        arrive(("lo", z))
        arrive(("hi", z))
        arrive(("ds", z))
        share(z, XY)

    def compute(z, xy):
        arrive(("c", z, xy))
        arrive(("cs", z, xy))
        at = slot(z, xy)
        lane = lax.broadcasted_iota(jnp.int32, (rows, sc.shape[2]), 1)
        routed_scale, shared_scale = [], []
        for core in range(2):
            columns = jnp.transpose(sc[at, core])
            routed_scale.append(
                jnp.sum(jnp.where(lane == e_at, columns, 0.0), axis=1, keepdims=True)
            )
            shared_scale.append(columns[:, sc.shape[2] - 1 :])
        routed_scale = jnp.concatenate(routed_scale, axis=0)
        shared_scale = jnp.concatenate(shared_scale, axis=0)
        inputs = tok[at].reshape(2 * rows, tok.shape[3])
        gate_part = jnp.dot(inputs, w_gate[...], preferred_element_type=jnp.float32)
        up_part = jnp.dot(inputs, w_up[...], preferred_element_type=jnp.float32)
        hidden = gate_part * jax.nn.sigmoid(gate_part) * up_part
        hidden = jnp.concatenate(
            [
                (hidden[:, :hidden_units] * routed_scale).astype(jnp.bfloat16),
                (hidden[:, hidden_units:] * shared_scale).astype(jnp.bfloat16),
            ],
            axis=1,
        )
        result = jnp.dot(hidden, w_down[...], preferred_element_type=jnp.float32)
        part[at] = result.astype(jnp.bfloat16).reshape(2, rows, tok.shape[3])
        send(("pc", z, xy), part.at[at, 1], from_core.at[at], "c")

    def f32(values):
        return values.astype(jnp.float32)

    def chip_sum(z, xy):
        arrive(("pc", z, xy))
        return f32(part[slot(z, xy), 0]) + f32(from_core[slot(z, xy)])

    def send_diagonal(z):
        at = slot(z, XY)
        part[at, 0] = chip_sum(z, XY).astype(jnp.bfloat16)
        low, high = pl.ds(0, half), pl.ds(half, half)
        send(("plo", z), part.at[at, 0, low], from_diag.at[z, low], "x")
        send(("phi", z), part.at[at, 0, high], from_diag.at[z, high], "y")

    def send_sides(z):
        arrive(("plo", z))
        arrive(("phi", z))
        total = chip_sum(z, X)
        part[slot(z, X), 0, :half] = total[:half].astype(jnp.bfloat16)
        part[slot(z, X), 0, half:] = (total[half:] + f32(from_diag[z, half:])).astype(jnp.bfloat16)
        send(("px", z), part.at[slot(z, X), 0], from_x.at[z], "x")
        total = chip_sum(z, Y)
        part[slot(z, Y), 0, :half] = (total[:half] + f32(from_diag[z, :half])).astype(jnp.bfloat16)
        part[slot(z, Y), 0, half:] = total[half:].astype(jnp.bfloat16)
        send(("py", z), part.at[slot(z, Y), 0], from_y.at[z], "y")

    def column_sum(z):
        total = chip_sum(z, NONE)
        arrive(("px", z))
        arrive(("py", z))
        return total + f32(from_x[z]) + f32(from_y[z])

    send_tokens("g", Z0, NONE, Z1, NONE, "z1")
    spread(Z0)
    send_tokens("g", Z0, NONE, Z2, NONE, "z2")
    for load in loads:
        load.wait()
    w_down[0:hidden_units, :] = jnp.transpose(down_raw[...])

    order = (Z0, Z1, Z2, Z12)
    for number, z in enumerate(order):
        compute(z, NONE)
        diagonal(z)
        if number + 1 < len(order):
            later = order[number + 1]
            tokens_arrive("g", later, NONE)
            if later == Z2:
                send_tokens("g", Z2, NONE, Z12, NONE, "z1")
            spread(later)
        compute(z, X)
        compute(z, Y)
        diagonal_arrives(z)
        compute(z, XY)
        if number:
            send_diagonal(order[number - 1])
    send_diagonal(Z12)

    send_sides(Z12)
    send_sides(Z2)
    part[slot(Z12, NONE), 0] = column_sum(Z12).astype(jnp.bfloat16)
    send(("pz", Z12), part.at[slot(Z12, NONE), 0], from_z.at[0], "z1")
    send_sides(Z1)
    total = column_sum(Z2)
    arrive(("pz", Z12))
    part[slot(Z2, NONE), 0] = (total + f32(from_z[0])).astype(jnp.bfloat16)
    send(("pz", Z2), part.at[slot(Z2, NONE), 0], from_z.at[1], "z2")
    send_sides(Z0)
    part[slot(Z1, NONE), 0] = column_sum(Z1).astype(jnp.bfloat16)
    send(("pz", Z1), part.at[slot(Z1, NONE), 0], from_z.at[2], "z1")
    total = column_sum(Z0)
    arrive(("pz", Z2))
    arrive(("pz", Z1))
    out_ref[...] = (total + f32(from_z[1]) + f32(from_z[2])).astype(out_ref.dtype)
    for copy in messages.values():
        copy.wait_send()


MESSAGES = 112


def fused_body(
    tokens,
    norm_gain,
    router_weight,
    shared_gate_vector,
    expert_ids,
    gate_weight,
    up_weight,
    down_weight,
    shared_gate_weight,
    shared_up_weight,
    shared_down_weight,
):
    rows, width = tokens.shape
    hidden_units = gate_weight.shape[2]
    shared_units = shared_gate_weight.shape[1] // lax.axis_size("dp")
    units = hidden_units + shared_units
    planes = 16
    anywhere = pl.BlockSpec(memory_space=pl.ANY)
    block = (rows, width)
    return pl.pallas_call(
        functools.partial(fused_kernel, rows, hidden_units, shared_units),
        out_shape=jax.ShapeDtypeStruct(block, jnp.bfloat16),
        in_specs=[pl.BlockSpec(memory_space=pltpu.VMEM)] * 5 + [anywhere] * 6,
        out_specs=pl.BlockSpec(memory_space=pltpu.VMEM),
        scratch_shapes=[
            pltpu.VMEM((planes, 2) + block, jnp.bfloat16),
            pltpu.VMEM((planes, 2, 8, rows), jnp.float32),
            pltpu.VMEM((planes, 2) + block, jnp.bfloat16),
            pltpu.VMEM((planes,) + block, jnp.bfloat16),
            pltpu.VMEM((4,) + block, jnp.bfloat16),
            pltpu.VMEM((4,) + block, jnp.bfloat16),
            pltpu.VMEM((4,) + block, jnp.bfloat16),
            pltpu.VMEM((3,) + block, jnp.bfloat16),
            pltpu.VMEM((width, units), jnp.bfloat16),
            pltpu.VMEM((width, units), jnp.bfloat16),
            pltpu.VMEM((width, hidden_units), jnp.bfloat16),
            pltpu.VMEM((units, width), jnp.bfloat16),
            pltpu.SemaphoreType.DMA((MESSAGES,)),
            pltpu.SemaphoreType.DMA((MESSAGES,)),
            pltpu.SemaphoreType.DMA((6,)),
        ],
        compiler_params=pltpu.CompilerParams(
            collective_id=0, has_side_effects=True, vmem_limit_bytes=VMEM_LIMIT
        ),
    )(
        tokens,
        norm_gain,
        router_weight,
        shared_gate_vector,
        expert_ids,
        gate_weight,
        up_weight,
        down_weight,
        shared_gate_weight,
        shared_up_weight,
        shared_down_weight,
    )


def solution(mesh):
    fused = (mesh.shape["expert"], mesh.shape["dp"]) == (1 << 2, 1 << 3)
    return jax.shard_map(
        fused_body if fused else body,
        mesh=mesh,
        in_specs=(
            P(("expert", "dp"), None),
            P(),
            P(),
            P(),
            P(("expert", "dp"), None),
            P("expert", None, "dp"),
            P("expert", None, "dp"),
            P("expert", None, "dp"),
            P(None, "expert"),
            P(None, "expert"),
            P("expert", None),
        ),
        out_specs=P(("expert", "dp"), None),
        check_vma=False,
    )
```
